128 devices in a mesh: tp: 16 (over x_lo, z, core), seq: 8 (over y, x_hi).
Axes of the slice: x: 4 (x_hi: 2, x_lo: 2; x = x_hi * 2 + x_lo), y: 4, z: 4, core: 2. Of those that a mesh axis runs over, the one named last changes fastest.
Arguments:
- residual: bfloat16 [2048, 4096], P('seq'), may hold values from -6 to 6
- mix_gain: float32 [4096], replicated, may hold values from 0.5 to 1.5
- in_proj: bfloat16 [4096, 4096], P(None, 'tp'), may hold values from -0.09375 to 0.09375
- branch_proj: bfloat16 [4096, 4096], P(None, 'tp'), may hold values from -0.09375 to 0.09375
- conv_weight: float32 [4, 4096], P(None, 'tp'), may hold values from -3 to 3
- conv_bias: float32 [4096], P('tp'), may hold values from -1.25 to 1.25
- input_gate: bfloat16 [16, 256, 256], P('tp'), may hold values from -0.375 to 0.375
- input_bias: float32 [4096], P('tp'), may hold values from -3 to 3
- decay_gate: bfloat16 [16, 256, 256], P('tp'), may hold values from -0.375 to 0.375
- decay_bias: float32 [4096], P('tp'), may hold values from -3 to 3
- decay_param: float32 [4096], P('tp'), may hold values from -13 to -2, as said below
- out_proj: bfloat16 [4096, 4096], P('tp'), may hold values from -0.25 to 0.25
- mlp_gain: float32 [4096], replicated, may hold values from 0.5 to 1.5
- gate_proj: bfloat16 [4096, 12288], P('seq', 'tp'), may hold values from -0.09375 to 0.09375
- up_proj: bfloat16 [4096, 12288], P('seq', 'tp'), may hold values from -0.09375 to 0.09375
- down_proj: bfloat16 [12288, 4096], P('tp'), may hold values from -0.078125 to 0.078125
Outputs:
- updated: bfloat16 [2048, 4096], P('seq')
The draws below stay inside these ranges and needn't reach their ends.
Inputs may be any that keep to these rules, and one draw needn't show every extreme that they name: softplus(decay_param) lies between 0.02 / 2048 and 0.1 for every channel.
All inputs are finite; a program needn't handle non-finite values.
Results may differ from the reference program's by a relative error of at most 0.02.
Values may be sent and summed in bfloat16 or wider, within the bound.
A program may use at most 128 MiB of HBM per device.

```python
import jax
import jax.numpy as jnp
from jax import lax

D = 4096
LRU = 4096
FF = 12288
HEADS = 16
CONV = 4
HEAD = 256
TOKENS = 2048


def draw_decay_param(key, part):
    lowest = 0.02 / TOKENS
    highest = 0.1
    spread = jax.random.uniform(key, (LRU,), jnp.float32)
    rate = lowest * jnp.exp(spread * jnp.log(highest / lowest))
    return jnp.log(jnp.expm1(rate)).astype(jnp.float32)


def raised(values, rng, source, target, shards_of, factor):
    owner, partner = [(jnp.arange(values.shape[axis_at]) // (values.shape[axis_at] // shards_of)).reshape([-1 if axis == axis_at else 1 for axis in range(values.ndim)]) for axis_at in (source, target)]
    chosen = jax.random.permutation(rng, shards_of)[partner]
    strong = (owner == chosen) | (owner == (partner + shards_of // 2) % shards_of)
    return jnp.where(strong, factor * values, values)


def steps_of(own_key, shape, shards, low, top_value):
    level = 1.0
    for axis_at, shards_of in shards:
        heights = jax.random.uniform(jax.random.fold_in(jax.random.fold_in(own_key, 6), axis_at), (shards_of,), jnp.float32, low / len(shards), top_value / len(shards))
        level = level * jnp.repeat(jnp.exp(heights), shape[axis_at] // shards_of).reshape((-1,) + (1,) * (len(shape) - 1 - axis_at))
    return level


def scatter_about(own_key, dims, deviation, bound, shards=(), dtype=jnp.bfloat16):
    values = jax.random.normal(own_key, dims, jnp.float32) * deviation
    if len(shards) > 0:
        values = steps_of(own_key, dims, shards, -0.22, 0.18) * values
    return jnp.clip(values, min=-bound, max=bound).astype(dtype)


def noise_with(own_key, extent, scale, most, cuts, heavy, dtype=jnp.bfloat16):
    drawn = scale * jax.random.normal(own_key, extent, jnp.float32)
    if cuts:
        drawn = drawn * steps_of(own_key, extent, cuts, -0.22, 0.18)
    return jnp.clip(raised(drawn, jax.random.fold_in(own_key, 3), *heavy), -most, most).astype(dtype)


def setup_inputs(seed: int = 0) -> dict:
    seeds = jax.random.split(jax.random.key(seed), 17)
    residual = scatter_about(seeds[0], (TOKENS, D), 1.0, 6.0, ((0, 8),))
    mix_gain = jnp.clip(1.0 + 0.1 * jax.random.normal(seeds[1], (D,), jnp.float32), 0.5, 1.5)
    in_proj = scatter_about(seeds[2], (D, LRU), D ** -0.5, 0.09375, ((1, 16),))
    branch_proj = scatter_about(seeds[3], (D, LRU), D ** -0.5, 0.09375, ((1, 16),))
    conv_weight = scatter_about(seeds[4], (CONV, LRU), CONV ** -0.5, 3.0, ((1, 16),), jnp.float32)
    conv_bias = scatter_about(seeds[5], (LRU,), 0.2, 1.25, ((0, 16),), jnp.float32)
    input_gate = scatter_about(seeds[6], (HEADS, HEAD, HEAD), HEAD ** -0.5, 0.375, ((0, 16),))
    input_bias = scatter_about(seeds[7], (LRU,), 0.5, 3.0, ((0, 16),), jnp.float32)
    decay_gate = scatter_about(seeds[8], (HEADS, HEAD, HEAD), HEAD ** -0.5, 0.375, ((0, 16),))
    decay_bias = scatter_about(seeds[9], (LRU,), 0.5, 3.0, ((0, 16),), jnp.float32)
    decay_param = draw_decay_param(jax.random.fold_in(seeds[16], 71), 0)
    out_proj = noise_with(seeds[11], (LRU, D), (LRU // 4) ** -0.5, 0.25, ((0, 16),), (0, 1, 16, 2.0))
    mlp_gain = jnp.clip(1.0 + 0.1 * jax.random.normal(seeds[12], (D,), jnp.float32), 0.5, 1.5)
    gate_proj = scatter_about(seeds[13], (D, FF), D ** -0.5, 0.09375, ((0, 8), (1, 16)))
    up_proj = scatter_about(seeds[14], (D, FF), D ** -0.5, 0.09375, ((0, 8), (1, 16)))
    down_proj = noise_with(seeds[15], (FF, D), FF ** -0.5, 0.078125, ((0, 16),), (0, 1, 16, 2.0))
    return {"residual": residual, "mix_gain": mix_gain, "in_proj": in_proj, "branch_proj": branch_proj, "conv_weight": conv_weight, "conv_bias": conv_bias, "input_gate": input_gate, "input_bias": input_bias, "decay_gate": decay_gate, "decay_bias": decay_bias, "decay_param": decay_param, "out_proj": out_proj, "mlp_gain": mlp_gain, "gate_proj": gate_proj, "up_proj": up_proj, "down_proj": down_proj}


epsilon = 1e-06

def rms_norm(values, gain):
    wide = values.astype(jnp.float32)
    factor = lax.rsqrt(lax.optimization_barrier(jnp.mean(wide * wide, axis=-1, keepdims=True)) + epsilon)
    return (wide * factor * gain).astype(jnp.bfloat16)

def block_gates(values, weight, bias):
    heads, width = (weight.shape[0], weight.shape[1])
    grouped = values.reshape(values.shape[0], heads, width).astype(jnp.float32)
    mixed = jnp.einsum('thi,hij->thj', grouped, weight.astype(jnp.float32))
    return jax.nn.sigmoid(mixed.reshape(values.shape[0], heads * width) + bias)

def smooth(inner, tail, conv_weight, conv_bias):
    taps = conv_weight.shape[0]
    length = inner.shape[0]
    padded = jnp.concatenate([tail, inner], axis=0).astype(jnp.float32)
    total = conv_bias + jnp.zeros((length, inner.shape[1]), jnp.float32)
    for offset in range(taps):
        total = total + conv_weight[offset] * padded[taps - 1 - offset:taps - 1 - offset + length]
    return lax.optimization_barrier(total.astype(jnp.bfloat16))

def advance(state, pair):
    state = pair[0] * state + pair[1]
    return (state, state)

def reference(residual, mix_gain, in_proj, branch_proj, conv_weight, conv_bias, input_gate, input_bias, decay_gate, decay_bias, decay_param, out_proj, mlp_gain, gate_proj, up_proj, down_proj):
    taps = conv_weight.shape[0]
    normed = rms_norm(residual, mix_gain)
    branch = jax.nn.gelu(jnp.dot(normed, branch_proj, preferred_element_type=jnp.float32), approximate=True)
    inner = jnp.dot(normed, in_proj, preferred_element_type=jnp.float32).astype(jnp.bfloat16)
    tail = jnp.zeros((taps - 1, inner.shape[1]), jnp.bfloat16)
    smoothed = smooth(inner, tail, conv_weight, conv_bias)
    input_rate = block_gates(smoothed, input_gate, input_bias)
    decay_rate = block_gates(smoothed, decay_gate, decay_bias)
    log_decay = -8.0 * decay_rate * jax.nn.softplus(decay_param)
    decay = jnp.exp(log_decay)
    first = (jnp.arange(TOKENS) == 0)[:, None]
    scale_in = jnp.where(first, 1.0, jnp.sqrt(-jnp.expm1(2.0 * log_decay)))
    pushed = smoothed.astype(jnp.float32) * input_rate * scale_in
    _, states = lax.scan(advance, jnp.zeros((LRU,), jnp.float32), (decay, pushed))
    gated = (states * branch).astype(jnp.bfloat16)
    mixed = jnp.dot(gated, out_proj, preferred_element_type=jnp.float32)
    middle = lax.optimization_barrier((residual.astype(jnp.float32) + mixed).astype(jnp.bfloat16))
    hidden_in = rms_norm(middle, mlp_gain)
    gate = jnp.dot(hidden_in, gate_proj, preferred_element_type=jnp.float32)
    up = jnp.dot(hidden_in, up_proj, preferred_element_type=jnp.float32)
    hidden = (jax.nn.gelu(gate, approximate=True) * up).astype(jnp.bfloat16)
    output = jnp.dot(hidden, down_proj, preferred_element_type=jnp.float32)
    return (middle.astype(jnp.float32) + output).astype(jnp.bfloat16)
```

```python
import math

import jax
import jax.numpy as jnp
from jax import lax
from jax.experimental import pallas as pl
from jax.experimental.pallas import tpu as pltpu
from jax.sharding import Mesh
from jax.sharding import PartitionSpec as P

SEQ = ("y", "x_hi")
TP = ("x_lo", "z", "core")
AXES = ("x_lo", "z", "core", "y", "x_hi")
BF = jnp.bfloat16
F32 = jnp.float32
EPS = 1e-06

ROWS = 256
D = 4096
HALF = D // 2
WIDTH = 256
FF = 768
PIECE = 16
CHUNK = 256
CHUNKS = FF // CHUNK
DEPTH = 512
SLOTS = 96


def gelu(v):
    return 0.5 * v * (1.0 + jnp.tanh(math.sqrt(2.0 / math.pi) * (v + 0.044715 * v * v * v)))


def one_less_exp(v):
    series = 1.0 + v / 8.0
    for n in (7.0, 6.0, 5.0, 4.0, 3.0, 2.0):
        series = 1.0 + v / n * series
    return jnp.where(v > -0.25, -v * series, 1.0 - jnp.exp(v))


def softplus(v):
    t = jnp.exp(-jnp.abs(v))
    series = 1.0 / 7.0 - t / 8.0
    for n in (6.0, 5.0, 4.0, 3.0, 2.0, 1.0):
        series = 1.0 / n - t * series
    return jnp.maximum(v, 0.0) + jnp.where(t < 0.05, t * series, jnp.log(1.0 + t))


def kernel(
    residual_h, mix_gain, in_h, branch_h, conv_w, conv_b, input_gate, input_bias, decay_gate, decay_bias,
    decay_param, out_proj_h, mlp_gain, gate_h, up_h, down_h,
    updated,
    res, w_in, w_branch, w_out, w_down, w_gate, w_up,
    normed, inner, branch, tail, pad, decays, states, sum_out, sums, gated,
    part, near, halved, xa, s2a, za, zb, s2b, xb,
    middle, hid_out, hid, gate_out, up_out, gate_mid, up_mid, gate_in, up_in, gate_own, up_own, hidden, final,
    loc, send, recv,
):
    x_lo, z, core, y, x_hi = (lax.axis_index(a) for a in AXES)
    position = y * 2 + x_hi
    x = x_hi * 2 + x_lo

    def at_x(step):
        there = lax.rem(x + step, 4)
        return {"x_hi": there // 2, "x_lo": lax.rem(there, 2)}

    def at_y(step):
        return {"y": lax.rem(y + step, 4)}

    def at_z(step):
        return {"z": lax.rem(z + step, 4)}

    def at_seq(step):
        there = lax.rem(position + step, 8)
        return {"y": there // 2, "x_hi": lax.rem(there, 2)}

    at_core = {"core": 1 - core}
    at_pair = {"x_lo": 1 - x_lo}
    at_hi = {"x_hi": 1 - x_hi}

    used = [0]
    started = []

    def remote(src, dst, where):
        n = used[0]
        used[0] += 1
        return pltpu.make_async_remote_copy(
            src_ref=src, dst_ref=dst, send_sem=send.at[n], recv_sem=recv.at[n],
            device_id=where, device_id_type=pl.DeviceIdType.MESH,
        )

    def go(*copies):
        for copy in copies:
            copy.start()
            started.append(copy)

    def local(n, src, dst):
        copy = pltpu.make_async_copy(src, dst, loc.at[n])
        copy.start()
        return copy

    my_rows = pl.ds(pl.multiple_of(y * DEPTH, DEPTH), DEPTH)
    load_res = local(0, residual_h, res)
    load_in = local(1, in_h, w_in)
    load_branch = local(2, branch_h, w_branch)

    barrier = pltpu.get_barrier_semaphore()
    partners = [at_core, at_x(1), at_x(3), at_z(1), at_z(2), at_z(3)] + [at_seq(s) for s in range(1, 8)]
    for where in partners:
        pl.semaphore_signal(barrier, inc=1, device_id=where, device_id_type=pl.DeviceIdType.MESH)

    load_res.wait()

    @pl.loop(0, ROWS // PIECE)
    def _(i):
        rows = pl.ds(pl.multiple_of(i * PIECE, PIECE), PIECE)
        wide = res[rows, :].astype(F32)
        factor = lax.rsqrt(jnp.mean(wide * wide, axis=-1, keepdims=True) + EPS)
        normed[rows, :] = (wide * factor * mix_gain[...]).astype(BF)

    pl.semaphore_wait(barrier, len(partners))

    up_y, down_y = at_y(1), at_y(3)
    back = [pl.ds(pl.multiple_of(lax.rem(y + s, 4) * DEPTH, DEPTH), DEPTH) for s in range(4)]
    cols = [pl.ds(c * CHUNK, CHUNK) for c in range(CHUNKS)]
    own_gate_up = [remote(gate_h.at[:, cols[c]], w_gate.at[my_rows, cols[c]], up_y) for c in range(CHUNKS)]
    own_up_up = [remote(up_h.at[:, cols[c]], w_up.at[my_rows, cols[c]], up_y) for c in range(CHUNKS)]
    own_gate_down = [remote(gate_h.at[:, cols[c]], w_gate.at[my_rows, cols[c]], down_y) for c in range(CHUNKS)]
    own_up_down = [remote(up_h.at[:, cols[c]], w_up.at[my_rows, cols[c]], down_y) for c in range(CHUNKS)]
    pass_gate = [
        remote(w_gate.at[back[3], cols[c]], w_gate.at[back[3], cols[c]], up_y) for c in range(CHUNKS)
    ]
    pass_up = [remote(w_up.at[back[1], cols[c]], w_up.at[back[1], cols[c]], down_y) for c in range(CHUNKS)]

    go(own_gate_up[0], own_up_down[0])

    load_gate = local(5, gate_h, w_gate.at[my_rows, :])
    load_up = local(6, up_h, w_up.at[my_rows, :])
    load_out = local(3, out_proj_h, w_out)
    load_down = local(4, down_h, w_down)

    load_in.wait()
    inner_f32 = jnp.dot(normed[...], w_in[...], preferred_element_type=F32).astype(BF)
    inner[...] = inner_f32
    send_tail = remote(inner.at[pl.ds(ROWS - 16, 16), :], tail, at_seq(1))
    go(send_tail)
    pad[pl.ds(8, ROWS), :] = inner_f32.astype(F32)
    go(own_up_up[0], own_gate_down[0])

    load_branch.wait()
    branch[...] = gelu(jnp.dot(normed[...], w_branch[...], preferred_element_type=F32))

    send_tail.wait_recv()
    before = tail[...].astype(F32)[8:16, :]
    pad[pl.ds(0, 8), :] = jnp.where(position == 0, 0.0, before)

    total = conv_b[...] + jnp.zeros((ROWS, WIDTH), F32)
    for k in range(4):
        total = total + conv_w[pl.ds(k, 1), :] * pad[pl.ds(8 - k, ROWS), :]
    smoothed = total.astype(BF)
    input_rate = jax.nn.sigmoid(
        jnp.dot(smoothed, input_gate[0], preferred_element_type=F32) + input_bias[...]
    )
    decay_rate = jax.nn.sigmoid(
        jnp.dot(smoothed, decay_gate[0], preferred_element_type=F32) + decay_bias[...]
    )
    log_decay = -8.0 * decay_rate * softplus(decay_param[...])
    row = lax.broadcasted_iota(jnp.int32, (ROWS, WIDTH), 0)
    scale_in = jnp.sqrt(one_less_exp(2.0 * log_decay))
    scale_in = jnp.where(jnp.logical_and(row == 0, position == 0), 1.0, scale_in)
    a = jnp.exp(log_decay)
    b = smoothed.astype(F32) * input_rate * scale_in
    step = 1
    while step < ROWS:
        a_before = jnp.where(row < step, 1.0, pltpu.roll(a, step, 0))
        b_before = jnp.where(row < step, 0.0, pltpu.roll(b, step, 0))
        b = a * b_before + b
        a = a * a_before
        step *= 2
    decays[...] = a
    states[...] = b
    sum_out[...] = jnp.zeros((8, WIDTH), F32)
    sum_out[pl.ds(0, 1), :] = a[ROWS - 1 :, :]
    sum_out[pl.ds(1, 1), :] = b[ROWS - 1 :, :]
    send_sums = [remote(sum_out, sums.at[s], at_seq(s)) for s in range(1, 8)]
    go(*send_sums)

    own_gate_up[0].wait_recv()
    own_up_down[0].wait_recv()
    go(pass_gate[0], pass_up[0])
    go(own_gate_up[1], own_up_down[1], own_up_up[1], own_gate_down[1])

    for copy in send_sums:
        copy.wait_recv()
    carried = jnp.zeros((1, WIDTH), F32)
    for s in range(7, 0, -1):
        moved = sums[s, pl.ds(0, 1), :] * carried + sums[s, pl.ds(1, 1), :]
        carried = jnp.where(position >= s, moved, carried)
    gated[...] = ((states[...] + decays[...] * carried) * branch[...]).astype(BF)

    first, second = pl.ds(0, HALF), pl.ds(HALF, HALF)

    def partial_products(turn, lhs, weights, base):
        @pl.loop(0, HALF // 512)
        def _(i):
            columns = pl.ds(pl.multiple_of(base + i * 512, 512), 512)
            product = jnp.dot(lhs[...], weights[:, columns], preferred_element_type=F32)
            part[turn, :, :, :, :, columns] = product.astype(BF).reshape(2, 2, 4, PIECE, 512)

    def sum_over_tp(turn, lhs, weights, between):
        there = 1 - core
        swap = []
        for half in (first, second):
            partial_products(turn, lhs, weights, 0 if half is first else HALF)
            copy = remote(part.at[turn, there, :, :, :, half], near.at[turn, :, :, :, half], at_core)
            go(copy)
            swap.append(copy)

        def add_near(half):
            @pl.loop(0, 8)
            def _(i):
                xl, zz = i // 4, lax.rem(i, 4)
                halved[turn, xl, zz, :, half] = (
                    part[turn, core, xl, zz, :, half].astype(F32) + near[turn, xl, zz, :, half].astype(F32)
                ).astype(BF)

        swap[0].wait_recv()
        add_near(first)
        across = remote(halved.at[turn, 1 - x_lo, :, :, first], xa.at[turn], at_pair)
        go(across)
        swap[1].wait_recv()
        add_near(second)
        around = [
            remote(halved.at[turn, :, lax.rem(z + s, 4), :, second], zb.at[turn, s - 1], at_z(s))
            for s in (1, 3, 2)
        ]
        go(*around)
        between()
        across.wait_recv()

        @pl.loop(0, 4)
        def _(i):
            s2a[turn, i] = (
                halved[turn, x_lo, i, :, first].astype(F32) + xa[turn, i].astype(F32)
            ).astype(BF)

        around_a = [
            remote(s2a.at[turn, lax.rem(z + s, 4)], za.at[turn, s - 1], at_z(s)) for s in (1, 3, 2)
        ]
        go(*around_a)
        for copy in around:
            copy.wait_recv()

        @pl.loop(0, 2)
        def _(i):
            whole = halved[turn, i, z, :, second].astype(F32)
            for s in range(3):
                whole = whole + zb[turn, s, i].astype(F32)
            s2b[turn, i] = whole.astype(BF)

        across_b = remote(s2b.at[turn, 1 - x_lo], xb.at[turn], at_pair)
        go(across_b)
        for copy in around_a:
            copy.wait_recv()
        left = s2a[turn, z].astype(F32)
        for s in range(3):
            left = left + za[turn, s].astype(F32)
        across_b.wait_recv()
        right = s2b[turn, x_lo].astype(F32) + xb[turn].astype(F32)
        return left, right

    load_out.wait()

    def pass_second():
        own_gate_up[1].wait_recv()
        own_up_down[1].wait_recv()
        go(pass_gate[1], pass_up[1])
        go(own_gate_up[2], own_up_down[2], own_up_up[2], own_gate_down[2])

    left, right = sum_over_tp(0, gated, w_out, pass_second)
    mine = pl.ds(pl.multiple_of(core * 128 + x_lo * 64 + z * PIECE, PIECE), PIECE)
    middle[:, first] = (res[mine, first].astype(F32) + left).astype(BF)
    middle[:, second] = (res[mine, second].astype(F32) + right).astype(BF)
    wide = middle[...].astype(F32)
    factor = lax.rsqrt(jnp.mean(wide * wide, axis=-1, keepdims=True) + EPS)
    wide = (wide * factor * mlp_gain[...]).astype(BF)

    for i in range(4):
        even = wide[:, 2 * i * DEPTH : (2 * i + 1) * DEPTH]
        odd = wide[:, (2 * i + 1) * DEPTH : (2 * i + 2) * DEPTH]
        block = pl.ds(i * DEPTH, DEPTH)
        hid[x_hi, core, x_lo, z, :, block] = jnp.where(x_hi == 0, even, odd)
        hid_out[:, block] = jnp.where(x_hi == 0, odd, even)

    def gather_over_tp(own_a, own_b, enter):
        z_a = [remote(own_a(core, x_lo, z), own_a(core, x_lo, z), at_z(s)) for s in (1, 3, 2)]
        go(*z_a)
        enter()
        x_b = remote(own_b(core, x_lo, z), own_b(core, x_lo, z), at_pair)
        go(x_b)
        for copy in z_a:
            copy.wait_recv()
        everything = slice(None)
        x_a = remote(own_a(core, x_lo, everything), own_a(core, x_lo, everything), at_pair)
        c_a = remote(own_a(core, x_lo, everything), own_a(core, x_lo, everything), at_core)
        go(x_a, c_a)
        x_b.wait_recv()
        z_b = [remote(own_b(core, everything, z), own_b(core, everything, z), at_z(s)) for s in (1, 3, 2)]
        go(*z_b)
        x_a.wait_recv()
        c_a2 = remote(own_a(core, 1 - x_lo, everything), own_a(core, 1 - x_lo, everything), at_core)
        go(c_a2)
        for copy in z_b:
            copy.wait_recv()
        c_b = remote(own_b(core, everything, everything), own_b(core, everything, everything), at_core)
        go(c_b)
        return c_a, c_a2, c_b

    to_hi = remote(hid_out, hid.at[x_hi, core, x_lo, z], at_hi)
    go(to_hi)
    last = gather_over_tp(
        lambda c, l, k: hid.at[x_hi, c, l, k],
        lambda c, l, k: hid.at[1 - x_hi, c, l, k],
        to_hi.wait_recv,
    )
    own_gate_up[2].wait_recv()
    own_up_down[2].wait_recv()
    go(pass_gate[2], pass_up[2])
    for copy in last:
        copy.wait_recv()

    load_gate.wait()
    load_up.wait()
    gate_hop, up_hop, gate_last, up_last = [], [], [], []
    for c in range(CHUNKS):
        gate_hop.append(remote(gate_out.at[c], gate_mid.at[c], at_x(1)))
        up_hop.append(remote(up_out.at[c], up_mid.at[c], at_x(3)))
        gate_last.append(remote(gate_mid.at[c], gate_in.at[c], at_x(1)))
        up_last.append(remote(up_mid.at[c], up_in.at[c], at_x(3)))

    def features(group, weights, c):
        lhs = hid[group].reshape(ROWS, HALF)
        return jnp.dot(lhs, weights[:, cols[c]], preferred_element_type=F32)

    for c in range(CHUNKS):
        for copy in (own_up_up[c], own_gate_down[c], pass_gate[c], pass_up[c]):
            copy.wait_recv()
        gate_out[c] = features(1 - x_hi, w_gate, c).astype(BF)
        go(gate_hop[c])
        up_out[c] = features(1 - x_hi, w_up, c).astype(BF)
        go(up_hop[c])
        gate_own[:, cols[c]] = features(x_hi, w_gate, c)
        up_own[:, cols[c]] = features(x_hi, w_up, c)
    for c in range(CHUNKS):
        gate_hop[c].wait_recv()
        up_hop[c].wait_recv()
        go(gate_last[c], up_last[c])
    for c in range(CHUNKS):
        gate_last[c].wait_recv()
        up_last[c].wait_recv()
        gate = gate_own[:, cols[c]] + gate_in[c].astype(F32)
        up = up_own[:, cols[c]] + up_in[c].astype(F32)
        hidden[:, cols[c]] = (gelu(gate) * up).astype(BF)

    load_down.wait()
    left, right = sum_over_tp(1, hidden, w_down, lambda: None)
    final[core, x_lo, z, :, first] = (middle[:, first].astype(F32) + left).astype(BF)
    final[core, x_lo, z, :, second] = (middle[:, second].astype(F32) + right).astype(BF)
    last = gather_over_tp(
        lambda c, l, k: final.at[c, l, k, :, first] if not isinstance(k, slice) else final.at[c, l, :, :, first],
        lambda c, l, k: (
            final.at[c, l, k, :, second]
            if not isinstance(l, slice)
            else (final.at[c, :, k, :, second] if not isinstance(k, slice) else final.at[c, :, :, :, second])
        ),
        lambda: None,
    )
    stores = [local(7, final.at[core], updated.at[core])]
    for copy in last:
        copy.wait_recv()
    stores.append(local(8, final.at[1 - core], updated.at[1 - core]))
    for copy in stores:
        copy.wait()
    for copy in started:
        copy.wait_send()


def on_device(*args):
    vmem = pl.BlockSpec(memory_space=pltpu.VMEM)
    hbm = pl.BlockSpec(memory_space=pl.ANY)
    places = [hbm, vmem, hbm, hbm, vmem, vmem, vmem, vmem, vmem, vmem, vmem, hbm, vmem, hbm, hbm, hbm]
    args = [a.reshape(1, -1) if a.ndim == 1 else a for a in args]
    v = pltpu.VMEM
    scratch = [
        v((ROWS, D), BF), v((D, WIDTH), BF), v((D, WIDTH), BF), v((WIDTH, D), BF), v((FF, D), BF),
        v((4 * DEPTH, FF), BF), v((4 * DEPTH, FF), BF),
        v((ROWS, D), BF), v((ROWS, WIDTH), BF), v((ROWS, WIDTH), F32), v((16, WIDTH), BF),
        v((ROWS + 8, WIDTH), F32), v((ROWS, WIDTH), F32), v((ROWS, WIDTH), F32), v((8, WIDTH), F32),
        v((8, 8, WIDTH), F32), v((ROWS, WIDTH), BF),
        v((2, 2, 2, 4, PIECE, D), BF), v((2, 2, 4, PIECE, D), BF), v((2, 2, 4, PIECE, D), BF),
        v((2, 4, PIECE, HALF), BF), v((2, 4, PIECE, HALF), BF), v((2, 3, PIECE, HALF), BF),
        v((2, 3, 2, PIECE, HALF), BF), v((2, 2, PIECE, HALF), BF), v((2, PIECE, HALF), BF),
        v((PIECE, D), BF), v((PIECE, HALF), BF), v((2, 2, 2, 4, PIECE, HALF), BF),
        v((CHUNKS, ROWS, CHUNK), BF), v((CHUNKS, ROWS, CHUNK), BF), v((CHUNKS, ROWS, CHUNK), BF),
        v((CHUNKS, ROWS, CHUNK), BF), v((CHUNKS, ROWS, CHUNK), BF), v((CHUNKS, ROWS, CHUNK), BF),
        v((ROWS, FF), F32), v((ROWS, FF), F32), v((ROWS, FF), BF), v((2, 2, 4, PIECE, D), BF),
        pltpu.SemaphoreType.DMA((9,)), pltpu.SemaphoreType.DMA((SLOTS,)), pltpu.SemaphoreType.DMA((SLOTS,)),
    ]
    out = pl.pallas_call(
        kernel,
        name="layer",
        out_shape=jax.ShapeDtypeStruct((2, 2, 4, PIECE, D), BF),
        in_specs=places,
        out_specs=hbm,
        scratch_shapes=scratch,
        compiler_params=pltpu.CompilerParams(
            collective_id=0, has_side_effects=True, vmem_limit_bytes=60 * 1024 * 1024
        ),
    )(*args)
    return out.reshape(ROWS, D)


def solution(mesh):
    split = Mesh(mesh.devices.reshape(2, 4, 2, 4, 2), AXES)
    in_specs = (
        P(SEQ, None), P(), P(None, TP), P(None, TP), P(None, TP), P(TP), P(TP, None, None), P(TP),
        P(TP, None, None), P(TP), P(TP), P(TP, None), P(), P(SEQ, TP), P(SEQ, TP), P(TP, None),
    )
    return jax.shard_map(
        on_device, mesh=split, in_specs=in_specs, out_specs=P(SEQ, None), check_vma=False
    )
```
